32 devices in a mesh: layer: 4 (over x, core), grid: 8 (over z, y).
Axes of the slice: x: 2, y: 2, z: 4, core: 2. Of those that a mesh axis runs over, the one named last changes fastest.
Arguments:
- fourier: float32 [1024, 512, 256], P(('layer', 'grid')), may hold values from -6 to 6
- weights: float32 [1024], P(('layer', 'grid')), may hold values from 0.009375 to 0.09375
- legendre: float32 [256, 513, 1024], P('grid'), may hold values from -6 to 6
- pair_slots: int32 [256], replicated, may hold values from 0 to 255, each once
Outputs:
- spectra: float32 [256, 513, 256], P('grid', None, 'layer')
The draws below stay inside these ranges and needn't reach their ends.
Inputs may be any that keep to these rules, and one draw needn't show every extreme that they name: Each pair index appears exactly once; position q holds wavenumbers pair_slots[q] and 511 - pair_slots[q].
All inputs are finite; a program needn't handle non-finite values.
Results may differ from the reference program's by a relative error of at most 0.0003.
Values sent between devices are 32-bit elements; how exact they have to be, the bound alone decides.
A program may use at most 256 MiB of HBM per device.

```python
import math
import jax
import jax.numpy as jnp
from jax import lax

M = 512
J = 1024
C = 256
PAIRS = 256


def steps_of(rng, extent, shards, low, top_value):
    gain, own = 1.0, jax.random.fold_in(rng, 6)
    for position, shards_of in shards:
        steps = jnp.exp(jax.random.uniform(jax.random.fold_in(own, position), (shards_of,), jnp.float32, low / len(shards), top_value / len(shards)))
        gain = gain * jnp.repeat(steps, extent[position] // shards_of).reshape([-1 if axis == position else 1 for axis in range(len(extent))])
    return gain


def normal_values(own_key, extent, scale, reach, cuts=(), kind=jnp.bfloat16):
    values = scale * jax.random.normal(own_key, extent, jnp.float32)
    if cuts:
        values = values * steps_of(own_key, extent, cuts, -0.22, 0.18)
    return jnp.clip(values, -reach, reach).astype(kind)


def setup_inputs(seed: int = 0) -> dict:
    keys = jax.random.split(jax.random.key(seed), 5)
    fourier = normal_values(keys[0], (J, M, C), 1.0, 6.0, ((0, 32),), jnp.float32)
    weights = jnp.clip(jnp.exp(math.log(0.09375) - 2.3025851 * jax.random.uniform(keys[1], (J,), jnp.float32) ** steps_of(keys[1], (J,), ((0, 32),), -0.2, 0.2)), 0.009375, 0.09375)
    legendre = normal_values(keys[2], (PAIRS, M + 1, J), 1.0, 6.0, ((0, 8),), jnp.float32)
    pair_slots = jax.random.permutation(keys[3], PAIRS).astype(jnp.int32)
    return dict(fourier=fourier, weights=weights, legendre=legendre, pair_slots=pair_slots)


def reference(fourier, weights, legendre, pair_slots):
    scaled = fourier * weights[:, None, None]
    row_ids = jnp.arange(M + 1, dtype=jnp.int32)
    fields_count = scaled.shape[2]

    def pair_block(inputs):
        poly_block, slot_value = inputs
        wave_first = slot_value.astype(jnp.int32)
        wave_second = (M - 1 - slot_value).astype(jnp.int32)
        first_values = lax.dynamic_index_in_dim(scaled, wave_first, 1, keepdims=False)
        second_values = lax.dynamic_index_in_dim(scaled, wave_second, 1, keepdims=False)
        stacked = jnp.concatenate([first_values, second_values], axis=1)
        product = jnp.dot(poly_block, stacked, precision=lax.Precision.HIGHEST, preferred_element_type=jnp.float32)
        in_first = row_ids[:, None] < (M - wave_first)
        return jnp.where(in_first, product[:, :fields_count], product[:, fields_count:])

    return lax.map(pair_block, (legendre, pair_slots))
```

```python
import functools

import jax
import jax.numpy as jnp
from jax import lax
from jax.experimental import pallas as pl
from jax.experimental.pallas import tpu as pltpu
from jax.sharding import PartitionSpec as P

CHUNKS = (1, 6, 1)
LANES = 128


def pack_kernel(waves, half, slots_ref, x_ref, w_ref, *rest):
    o_ref = rest[-1]
    rows = w_ref.shape[0]
    scale = w_ref[...]
    in_low = lax.broadcasted_iota(jnp.int32, (rows, LANES), 1) < half

    def step(q, carry):
        a = slots_ref[q]
        first = x_ref[pl.ds(a, rows, stride=waves), :] * scale
        second = x_ref[pl.ds(waves - 1 - a, rows, stride=waves), :] * scale
        o_ref[0, q] = jnp.where(in_low, first, pltpu.roll(second, half, 1))
        o_ref[1, q] = jnp.where(in_low, pltpu.roll(first, half, 1), second)
        return carry

    lax.fori_loop(0, o_ref.shape[1], step, 0, unroll=8)


def pack(fourier, weights, slots, layers, after):
    lats, waves, fields = fourier.shape
    pairs = slots.shape[0]
    flat = fourier.reshape(lats * waves, fields)
    wide = jnp.broadcast_to(weights[:, None], (lats, LANES))
    tile = 8
    return pl.pallas_call(
        functools.partial(pack_kernel, waves, fields // layers),
        grid_spec=pltpu.PrefetchScalarGridSpec(
            num_scalar_prefetch=1,
            grid=(fields // LANES, lats // tile),
            in_specs=[
                pl.BlockSpec((tile * waves, LANES), lambda c, i, s: (i, c)),
                pl.BlockSpec((tile, LANES), lambda c, i, s: (i, 0)),
            ]
            + [pl.BlockSpec(memory_space=pl.ANY)] * len(after),
            out_specs=pl.BlockSpec((2, pairs, tile, LANES), lambda c, i, s: (c, 0, i, 0)),
        ),
        out_shape=jax.ShapeDtypeStruct((layers, pairs, lats, LANES), jnp.float32),
        compiler_params=pltpu.CompilerParams(vmem_limit_bytes=56 * 2**20),
        cost_estimate=pl.CostEstimate(flops=fourier.size * 4, bytes_accessed=fourier.size * 4 * 4, transcendentals=0),
        name="pack",
    )(slots, flat, wide, *after)


def split(x):
    high = x.astype(jnp.bfloat16)
    return high, (x - high.astype(jnp.float32)).astype(jnp.bfloat16)


def project_kernel(limit_ref, poly_ref, x_ref, *rest):
    o_ref = rest[-1]
    half = o_ref.shape[1]
    limit = limit_ref[pl.program_id(0)]
    x = x_ref[...].reshape(-1, LANES)
    right = jnp.concatenate(split(x), axis=1)
    high, low = split(poly_ref[0])
    product = jnp.dot(high, right, preferred_element_type=jnp.float32)
    product = product + jnp.dot(low, right, preferred_element_type=jnp.float32)
    total = (product[:, :LANES] + product[:, LANES:]).T
    rows = lax.broadcasted_iota(jnp.int32, (half, total.shape[1]), 1)
    o_ref[0] = jnp.where(rows < limit, total[:half], total[half:])


def project(legendre, owned, limits, start, so_far):
    pairs, degrees, lats = legendre.shape
    sources, count, part, _ = owned.shape
    half = LANES // 2
    in_specs = [
        pl.BlockSpec((1, degrees, lats), lambda q, s: (q + start, 0, 0)),
        pl.BlockSpec((sources, 1, part, LANES), lambda q, s: (0, q, 0, 0)),
    ]
    operands = [limits, legendre, owned]
    aliases = {}
    if so_far is not None:
        in_specs.append(pl.BlockSpec(memory_space=pl.ANY))
        operands.append(so_far)
        aliases = {3: 0}
    return pl.pallas_call(
        project_kernel,
        grid_spec=pltpu.PrefetchScalarGridSpec(
            num_scalar_prefetch=1,
            grid=(count,),
            in_specs=in_specs,
            out_specs=pl.BlockSpec((1, half, degrees), lambda q, s: (q + start, 0, 0)),
        ),
        out_shape=jax.ShapeDtypeStruct((pairs, half, degrees), jnp.float32),
        input_output_aliases=aliases,
        compiler_params=pltpu.CompilerParams(vmem_limit_bytes=56 * 2**20),
        cost_estimate=pl.CostEstimate(
            flops=count * degrees * lats * 1024, bytes_accessed=count * degrees * lats * 8, transcendentals=0
        ),
        name="project",
    )(*operands)


def shards(layers, grids, fourier, weights, legendre, pair_slots):
    local_pairs = legendre.shape[0]
    waves = 2 * pair_slots.shape[0]
    by_owner = pair_slots.reshape(grids, local_pairs)
    limits = waves - lax.dynamic_index_in_dim(by_owner, lax.axis_index("grid"), 0, keepdims=False)
    lats = fourier.shape[0]
    unit = local_pairs // sum(CHUNKS)
    start, outs = 0, [None]
    for step, size in enumerate(CHUNKS):
        count = size * unit
        chunk = by_owner[:, start : start + count].reshape(-1)
        packed = pack(fourier, weights, chunk, layers, [legendre, outs[step - 1]] if step > 1 else [])
        packed = packed.reshape(layers * grids, count, lats, LANES)
        owned = lax.all_to_all(packed, ("layer", "grid"), split_axis=0, concat_axis=0, tiled=True)
        outs.append(project(legendre, owned, limits[start : start + count], start, outs[-1]))
        start += count
    return outs[-1].transpose(0, 2, 1)


def solution(mesh):
    in_specs = (P(("layer", "grid"), None, None), P(("layer", "grid")), P("grid", None, None), P())
    out_specs = P("grid", None, "layer")
    body = functools.partial(shards, mesh.shape["layer"], mesh.shape["grid"])
    return jax.shard_map(body, mesh=mesh, in_specs=in_specs, out_specs=out_specs, check_vma=False)
```

```python
import functools

import jax
import jax.numpy as jnp
from jax import lax
from jax.experimental import pallas as pl
from jax.experimental.pallas import tpu as pltpu
from jax.sharding import PartitionSpec as P

LANES = 128


def pack_kernel(waves, half, local_pairs, begin, count, rows, slots_ref, x_ref, w_ref, *rest):
    o_ref, held, sem = rest[-3:]
    pitch = held.shape[1] // rows
    tiles = pl.num_programs(1)
    now = pl.program_id(0) * tiles + pl.program_id(1)
    last = pl.num_programs(0) * tiles - 1

    def copies(index, slot):
        columns = pl.ds(pl.multiple_of(index // tiles * LANES, LANES), LANES)
        for row in range(rows):
            start = pl.multiple_of((index % tiles * rows + row) * waves, 8)
            yield pltpu.make_async_copy(
                x_ref.at[pl.ds(start, waves), columns],
                held.at[slot, pl.ds(row * pitch, waves)],
                sem.at[slot, row],
            )

    @pl.when(now == 0)
    def _():
        for copy in copies(now, 0):
            copy.start()

    @pl.when(now < last)
    def _():
        for copy in copies(now + 1, (now + 1) % 2):
            copy.start()

    slot = now % 2
    for copy in copies(now, slot):
        copy.wait()

    x = held.at[slot]
    row_ids = lax.broadcasted_iota(jnp.int32, (rows, LANES), 0)
    scale = jnp.zeros((rows, LANES), jnp.float32)
    for row in range(rows):
        scale = jnp.where(row_ids == row, w_ref[pl.program_id(1) * rows + row], scale)
    in_low = lax.broadcasted_iota(jnp.int32, (rows, LANES), 1) < half

    def step(q, carry):
        a = slots_ref[q // count * local_pairs + begin + q % count]
        first = x[pl.ds(a, rows, stride=pitch), :] * scale
        second = x[pl.ds(waves - 1 - a, rows, stride=pitch), :] * scale
        o_ref[0, q] = jnp.where(in_low, first, pltpu.roll(second, half, 1))
        o_ref[1, q] = jnp.where(in_low, pltpu.roll(first, half, 1), second)
        return carry

    lax.fori_loop(0, o_ref.shape[1], step, 0, unroll=8)


def pack(fourier, weights, slots, layers, grids, begin, count, after):
    lats, waves, fields = fourier.shape
    pairs = grids * count
    local_pairs = slots.shape[0] // grids
    flat = fourier.reshape(lats * waves, fields)
    tile = 8
    return pl.pallas_call(
        functools.partial(pack_kernel, waves, fields // layers, local_pairs, begin, count, tile),
        grid_spec=pltpu.PrefetchScalarGridSpec(
            num_scalar_prefetch=1,
            grid=(fields // LANES, lats // tile),
            in_specs=[
                pl.BlockSpec(memory_space=pl.ANY),
                pl.BlockSpec(memory_space=pltpu.SMEM),
            ]
            + [pl.BlockSpec(memory_space=pl.ANY)] * len(after),
            out_specs=pl.BlockSpec((2, pairs, tile, LANES), lambda c, i, s: (c, 0, i, 0)),
            scratch_shapes=[
                pltpu.VMEM((2, tile * (waves + 8), LANES), jnp.float32),
                pltpu.SemaphoreType.DMA((2, tile)),
            ],
        ),
        out_shape=jax.ShapeDtypeStruct((layers, pairs, lats, LANES), jnp.float32),
        compiler_params=pltpu.CompilerParams(vmem_limit_bytes=56 * 2**20),
        cost_estimate=pl.CostEstimate(flops=fourier.size * 4, bytes_accessed=fourier.size * 4 * 4, transcendentals=0),
        name="pack",
    )(slots, flat, weights, *after)


def split(x):
    high = x.astype(jnp.bfloat16)
    return high, (x - high.astype(jnp.float32)).astype(jnp.bfloat16)


def project_kernel(limit_ref, poly_ref, x_ref, *rest):
    o_ref = rest[-1]
    half = o_ref.shape[1]
    limit = limit_ref[pl.program_id(0)]
    x = x_ref[...].reshape(-1, LANES)
    right = jnp.concatenate(split(x), axis=1)
    high, low = split(poly_ref[0])
    product = jnp.dot(high, right, preferred_element_type=jnp.float32)
    product = product + jnp.dot(low, right, preferred_element_type=jnp.float32)
    total = (product[:, :LANES] + product[:, LANES:]).T
    rows = lax.broadcasted_iota(jnp.int32, (half, total.shape[1]), 1)
    o_ref[0] = jnp.where(rows < limit, total[:half], total[half:])


def project(legendre, owned, limits, start, so_far):
    pairs, degrees, lats = legendre.shape
    sources, count, part, _ = owned.shape
    half = LANES // 2
    in_specs = [
        pl.BlockSpec((1, degrees, lats), lambda q, s: (q + start, 0, 0)),
        pl.BlockSpec((sources, 1, part, LANES), lambda q, s: (0, q, 0, 0)),
    ]
    operands = [limits, legendre, owned]
    aliases = {}
    if so_far is not None:
        in_specs.append(pl.BlockSpec(memory_space=pl.ANY))
        operands.append(so_far)
        aliases = {3: 0}
    return pl.pallas_call(
        project_kernel,
        grid_spec=pltpu.PrefetchScalarGridSpec(
            num_scalar_prefetch=1,
            grid=(count,),
            in_specs=in_specs,
            out_specs=pl.BlockSpec((1, half, degrees), lambda q, s: (q + start, 0, 0)),
        ),
        out_shape=jax.ShapeDtypeStruct((pairs, half, degrees), jnp.float32),
        input_output_aliases=aliases,
        compiler_params=pltpu.CompilerParams(vmem_limit_bytes=56 * 2**20),
        cost_estimate=pl.CostEstimate(
            flops=count * degrees * lats * 1024, bytes_accessed=count * degrees * lats * 8, transcendentals=0
        ),
        name="project",
    )(*operands)


def shards(layers, grids, fourier, weights, legendre, pair_slots):
    local_pairs = legendre.shape[0]
    waves = 2 * pair_slots.shape[0]
    by_owner = pair_slots.reshape(grids, local_pairs)
    limits = waves - lax.dynamic_index_in_dim(by_owner, lax.axis_index("grid"), 0, keepdims=False)
    lats = fourier.shape[0]
    first, last = max(1, local_pairs // 8), max(1, local_pairs * 3 // 32)
    start, outs = 0, [None]
    for step, count in enumerate((first, local_pairs - first - last, last)):
        after = [legendre, outs[step - 1]] if step > 1 else []
        packed = pack(fourier, weights, pair_slots, layers, grids, start, count, after)
        packed = packed.reshape(layers * grids, count, lats, LANES)
        owned = lax.all_to_all(packed, ("layer", "grid"), split_axis=0, concat_axis=0, tiled=True)
        outs.append(project(legendre, owned, limits[start : start + count], start, outs[-1]))
        start += count
    return outs[-1].transpose(0, 2, 1)


def solution(mesh):
    in_specs = (P(("layer", "grid"), None, None), P(("layer", "grid")), P("grid", None, None), P())
    out_specs = P("grid", None, "layer")
    body = functools.partial(shards, mesh.shape["layer"], mesh.shape["grid"])
    return jax.shard_map(body, mesh=mesh, in_specs=in_specs, out_specs=out_specs, check_vma=False)
```
